128 devices in a mesh: row: 8 (over y_hi, x), col: 16 (over z, y_lo, core).
Axes of the slice: x: 4, y: 4 (y_hi: 2, y_lo: 2; y = y_hi * 2 + y_lo), z: 4, core: 2. Of those that a mesh axis runs over, the one named last changes fastest.
Arguments:
- integrals: bfloat16 [2400, 2400, 256], P('row', 'col'), may hold values from -6 to 6
- occ_coef: bfloat16 [2400, 96], P('row'), may hold values from -0.125 to 0.125
- virt_coef: bfloat16 [2400, 2304], P('col'), may hold values from -0.125 to 0.125
- pair_index: int32 [256], replicated, may hold values from 0 to 255, each once
Outputs:
- transformed: bfloat16 [96, 2304, 256], P('row', 'col')
The draws below stay inside these ranges and needn't reach their ends.
Inputs may be any that keep to these rules, and one draw needn't show every extreme that they name: pair_index holds each of 0 to 255 once.
All inputs are finite; a program needn't handle non-finite values.
Results may differ from the reference program's by a relative error of at most 0.0049.
Values may be sent and summed in bfloat16 or wider, within the bound.
No kernel may reach another device: no remote copies, remote signals or barrier semaphores. Data moves between devices by JAX's collectives and lax.ppermute only.
A program may use at most 192 MiB of HBM per device.

```python
import jax
import jax.numpy as jnp
from jax import lax

O = 96
V = 2304
N = 2400
P_SIZE = 256


def block_scale(stream_key, shape, pieces, low, top_value):
    level = 1.0
    for position, blocks in pieces:
        heights = jax.random.uniform(jax.random.fold_in(jax.random.fold_in(stream_key, 6), position), (blocks,), jnp.float32, low / len(pieces), top_value / len(pieces))
        level = level * jnp.repeat(jnp.exp(heights), shape[position] // blocks).reshape((-1,) + (1,) * (len(shape) - 1 - position))
    return level


def centred(rng, shape, deviation, reach, shards=(), dtype=jnp.bfloat16):
    level = block_scale(rng, shape, shards, -0.22, 0.18) if shards else 1.0
    drawn = jax.random.normal(rng, shape, jnp.float32) * deviation * level
    return jnp.minimum(jnp.maximum(drawn, -reach), reach).astype(dtype)


def setup_inputs(seed: int = 0) -> dict:
    arg_keys = jax.random.split(jax.random.key(seed), 5)
    integrals = centred(arg_keys[0], (N, N, P_SIZE), 1.0, 6.0, ((0, 8), (1, 16)))
    occ_coef = centred(arg_keys[1], (N, O), N ** -0.5, 0.125, ((0, 8),))
    virt_coef = centred(arg_keys[2], (N, V), N ** -0.5, 0.125, ((0, 16),))
    pair_index = jax.random.permutation(arg_keys[3], P_SIZE).astype(jnp.int32)
    return {"integrals": integrals, "occ_coef": occ_coef, "virt_coef": virt_coef, "pair_index": pair_index}


def reference(integrals, occ_coef, virt_coef, pair_index):
    def one_pair(pair_block):
        half_rows = jnp.dot(occ_coef.T, pair_block, preferred_element_type=jnp.float32).astype(jnp.bfloat16)
        return jnp.dot(half_rows, virt_coef, preferred_element_type=jnp.float32).astype(jnp.bfloat16)

    slab_rows = lax.map(one_pair, jnp.moveaxis(integrals, 2, 0))
    chosen = jnp.take(slab_rows, pair_index.astype(jnp.int32), axis=0)
    return jnp.moveaxis(chosen, 0, 2)
```

```python
import jax
import jax.numpy as jnp
from jax import lax
from jax.sharding import PartitionSpec as P

F32, BF16 = jnp.float32, jnp.bfloat16
O_BLK = 12
A_BLK = 144
CHUNKS = (
    ((0, 40), (40, 80), (0, 256)),
    ((80, 112), (112, 150), (0, 256)),
)


def row_perm(mask):
    return [(i, i ^ mask) for i in range(8)]


def col_xor(mask):
    return [(i, i ^ mask) for i in range(16)]


def col_z(k):
    return [(i, (i + 4 * k) % 16) for i in range(16)]


def select_cols(mat, source):
    hot = (lax.broadcasted_iota(jnp.int32, (mat.shape[1], source.shape[0]), 0) == source[None, :]).astype(BF16)
    return jnp.dot(mat, hot, preferred_element_type=F32).astype(BF16)


def local(integrals, occ_coef, virt_coef, pair_index):
    r = lax.axis_index("row")
    c = lax.axis_index("col")
    yh, x = r // 4, r % 4
    z, yl, core = c // 4, (c // 2) % 2, c % 2

    pos = jnp.arange(96, dtype=jnp.int32)
    slot, j, t = pos // 24, (pos // O_BLK) % 2, pos % O_BLK

    def occ_source(order):
        k = sum(jnp.where(slot == s, order[s], 0) for s in range(4))
        return ((yh ^ j) * 4 + (x ^ k)) * O_BLK + t

    occ_both = select_cols(occ_coef, jnp.concatenate([occ_source((0, 3, 1, 2)), occ_source((0, 1, 3, 2))]))
    kinds = ((occ_both[:, :96], 1, 3), (occ_both[:, 96:], 3, 1))

    apos = jnp.arange(4 * A_BLK, dtype=jnp.int32)
    a_source = ((yl ^ ((apos // A_BLK) % 2)) * 2 + (core ^ (apos // (2 * A_BLK)))) * A_BLK + apos % A_BLK
    virt = []
    for k in range(4):
        cols = lax.dynamic_slice_in_dim(virt_coef, ((z + k) % 4) * 4 * A_BLK, 4 * A_BLK, axis=1)
        cols = select_cols(cols, a_source)
        virt.append(cols if k == 0 else lax.ppermute(cols, "col", col_z(k)))

    dots = {}
    for kind in (0, 1):
        for ch in CHUNKS:
            lo, hi = ch[kind]
            if (lo, hi, kind) not in dots:
                dots[lo, hi, kind] = jnp.einsum(
                    "mi,mnp->nip", kinds[kind][0], integrals[:, lo:hi], preferred_element_type=F32
                )

    acc = {}
    for ch in CHUNKS:
        p0, p1 = ch[2]
        parts = []
        for kind in (0, 1):
            lo, hi = ch[kind]
            _, first, second = kinds[kind]
            part = dots[lo, hi, kind][:, :, p0:p1]
            recv1 = lax.ppermute(part[:, 48:].astype(BF16), "row", row_perm(first))
            recv2 = lax.ppermute((part[:, 24:48] + recv1[:, 24:]).astype(BF16), "row", row_perm(second))
            parts.append(part[:, :24] + recv1[:, :24] + recv2)
        own = jnp.concatenate(parts, axis=0)
        own = jnp.swapaxes(own, 0, 1)
        recv3 = lax.ppermute(own[O_BLK:].astype(BF16), "row", row_perm(4))
        half = (own[:O_BLK] + recv3).astype(BF16)
        rows = [half] + [lax.ppermute(half, "col", col_z(k)) for k in (1, 2, 3)]
        rows = jnp.concatenate(rows, axis=1)
        cols = jnp.concatenate([v[lo:hi] for v in virt for lo, hi in ch[:2]], axis=0)
        prod = jnp.einsum("inp,na->iap", rows, cols, preferred_element_type=F32)
        acc[p0, p1] = acc[p0, p1] + prod if (p0, p1) in acc else prod

    out = 0.0
    for (p0, p1), total in acc.items():
        recv4 = lax.ppermute(total[:, 2 * A_BLK :].astype(BF16), "col", col_xor(1))
        recv5 = lax.ppermute(
            (total[:, A_BLK : 2 * A_BLK] + recv4[:, A_BLK:]).astype(BF16), "col", col_xor(2)
        )
        slab = (total[:, :A_BLK] + recv4[:, :A_BLK] + recv5).astype(BF16)
        hot = (lax.broadcasted_iota(jnp.int32, (p1 - p0, 256), 0) + p0 == pair_index[None, :]).astype(BF16)
        out = out + jnp.einsum("iap,pk->iak", slab, hot, preferred_element_type=F32)
    return out.astype(BF16)


def solution(mesh):
    return jax.shard_map(
        local,
        mesh=mesh,
        in_specs=(P("row", "col", None), P("row", None), P("col", None), P()),
        out_specs=P("row", "col", None),
        check_vma=False,
    )
```

```python
import jax
import jax.numpy as jnp
from jax import lax
from jax.experimental.layout import Layout, with_layout_constraint
from jax.sharding import PartitionSpec as P


F32, BF16 = jnp.float32, jnp.bfloat16
B = 12
A_BLK = 144
H = 128
CHUNKS = {"p": ("x", 0, 40), "q": ("y", 40, 88), "r": ("x", 88, 120, 150)}


def row_perm(mask):
    return [(i, i ^ mask) for i in range(8)]


def col_xor(mask):
    return [(i, i ^ mask) for i in range(16)]


def col_z(k):
    return [(i, (i + 4 * k) % 16) for i in range(16)]


def rowmajor(v):
    return with_layout_constraint(v, Layout(major_to_minor=tuple(range(v.ndim))))


def row(v, mask):
    return lax.ppermute(v, "row", row_perm(mask))


def select_cols(mat, source):
    hot = (lax.broadcasted_iota(jnp.int32, (mat.shape[1], source.shape[0]), 0) == source[None, :]).astype(BF16)
    return jnp.dot(mat, hot, preferred_element_type=F32).astype(BF16)


def f32(v):
    return v.astype(F32)


def x_first(d):
    a1 = row(d[2 * B : 6 * B, :, :H], 1)
    b1 = row(d[4 * B :, :, H:], 3)
    da, a1 = lax.optimization_barrier((d, a1))
    a2 = row((f32(da[6 * B :, :, :H]) + a1[2 * B :]).astype(BF16), 3)
    db, b1 = lax.optimization_barrier((d, b1))
    b2 = row((f32(db[2 * B : 4 * B, :, H:]) + b1[: 2 * B]).astype(BF16), 1)
    d, a2, b2 = lax.optimization_barrier((d, a2, b2))
    own = jnp.concatenate(
        [f32(d[: 2 * B, :, :H]) + a1[: 2 * B] + a2, f32(d[: 2 * B, :, H:]) + b1[2 * B :] + b2], axis=2
    )
    y = row(own[B:].astype(BF16), 4)
    return (own[:B] + y).astype(BF16)


def y_first(d, cols):
    y = row(d[4 * B :], 4)
    s = f32(d[: 4 * B]) + y
    a1 = row(s[B : 3 * B, :, :H].astype(BF16), 1)
    b1 = row(s[2 * B :, :, H:].astype(BF16), 3)
    s, a1, b1, *cols = lax.optimization_barrier((s, a1, b1, *cols))
    a2 = row((s[3 * B :, :, :H] + a1[B:]).astype(BF16), 3)
    b2 = row((s[B : 2 * B, :, H:] + b1[:B]).astype(BF16), 1)
    s, a2, b2 = lax.optimization_barrier((s, a2, b2))
    own = jnp.concatenate([s[:B, :, :H] + a1[:B] + a2, s[:B, :, H:] + b1[B:] + b2], axis=2)
    return own.astype(BF16), *cols


def local(integrals, occ_coef, virt_coef, pair_index):
    r = lax.axis_index("row")
    c = lax.axis_index("col")
    yh, x = r // 4, r % 4
    z, yl, core = c // 4, (c // 2) % 2, c % 2

    pos = jnp.arange(96, dtype=jnp.int32)
    source = {
        "x": ((yh ^ ((pos // B) % 2)) * 4 + (x ^ (pos // (2 * B)))) * B + pos % B,
        "y": ((yh ^ (pos // (4 * B))) * 4 + (x ^ ((pos // B) % 4))) * B + pos % B,
    }
    both = select_cols(occ_coef, jnp.concatenate([source["x"], source["y"]]))
    occ = {"x": both[:, :96], "y": both[:, 96:]}

    products, held = {}, occ_coef
    for name, (kind, *cuts) in CHUNKS.items():
        pieces = []
        for lo, hi in zip(cuts[:-1], cuts[1:]):
            weights = lax.optimization_barrier((occ[kind], held))[0]
            d = jnp.einsum("mi,mnp->inp", weights, integrals[:, lo:hi], preferred_element_type=F32).astype(BF16)
            held = rowmajor(d)
            pieces.append(held)
        products[name] = jnp.concatenate(pieces, axis=1)
    virt_coef = lax.optimization_barrier((virt_coef, held))[0]

    apos = jnp.arange(4 * A_BLK, dtype=jnp.int32)
    a_source = ((yl ^ ((apos // A_BLK) % 2)) * 2 + (core ^ (apos // (2 * A_BLK)))) * A_BLK + apos % A_BLK
    virt = {}
    for k in (0, 1, 3, 2):
        v = lax.dynamic_slice_in_dim(virt_coef, ((z + k) % 4) * 4 * A_BLK, 4 * A_BLK, axis=1)
        v = select_cols(v, a_source)
        virt[k] = v if k == 0 else lax.ppermute(v, "col", col_z(k))

    cols = {}
    for name, (_, *cuts) in CHUNKS.items():
        cols[name] = jnp.concatenate([virt[k][cuts[0] : cuts[-1]] for k in range(4)], axis=0)

    acc = 0.0
    for name, (kind, *_) in sorted(CHUNKS.items(), key=lambda item: item[1][0] == "x"):
        d = products[name]
        if kind == "x":
            half = x_first(d)
        else:
            names = tuple(cols)
            half, *tied = y_first(d, [cols[n] for n in names])
            cols = dict(zip(names, tied))
        h = [half] + [lax.ppermute(half, "col", col_z(k)) for k in (1, 2, 3)]
        acc = acc + jnp.einsum("inp,na->iap", jnp.concatenate(h, axis=1), cols[name], preferred_element_type=F32)

    r4 = lax.ppermute(acc[:, 2 * A_BLK :].astype(BF16), "col", col_xor(1))
    r5 = lax.ppermute((acc[:, A_BLK : 2 * A_BLK] + r4[:, A_BLK:]).astype(BF16), "col", col_xor(2))
    slab = (acc[:, :A_BLK] + r4[:, :A_BLK] + r5).astype(BF16)
    hot = (lax.broadcasted_iota(jnp.int32, (256, 256), 0) == pair_index[None, :]).astype(BF16)
    return jnp.einsum("iap,pk->iak", slab, hot, preferred_element_type=F32).astype(BF16)


def solution(mesh):
    return jax.shard_map(
        local,
        mesh=mesh,
        in_specs=(P("row", "col", None), P("row", None), P("col", None), P()),
        out_specs=P("row", "col", None),
        check_vma=False,
    )
```

```python
import jax
import jax.numpy as jnp
from jax import lax
from jax.experimental.layout import Layout, with_layout_constraint
from jax.sharding import PartitionSpec as P


F32, BF16 = jnp.float32, jnp.bfloat16
B = 12
A_BLK = 144
H = 128
CHUNKS = {"p": (0, 48), "r": (48, 104), "q": (104, 150)}


def row_perm(mask):
    return [(i, i ^ mask) for i in range(8)]


def col_xor(mask):
    return [(i, i ^ mask) for i in range(16)]


def rowmajor(v):
    return with_layout_constraint(v, Layout(major_to_minor=tuple(range(v.ndim))))


def row(v, mask):
    return lax.ppermute(v, "row", row_perm(mask))


def select_cols(mat, source):
    hot = (lax.broadcasted_iota(jnp.int32, (mat.shape[1], source.shape[0]), 0) == source[None, :]).astype(BF16)
    return jnp.dot(mat, hot, preferred_element_type=F32).astype(BF16)


def gather_z(half):
    return jnp.concatenate([half] + [lax.ppermute(half, "col", col_xor(4 * k)) for k in (1, 3, 2)], axis=1)


def f32(v):
    return v.astype(F32)


def x_first(d, cols):
    a1 = row(d[2 * B : 6 * B, :, :H], 1)
    b1 = row(d[4 * B :, :, H:], 3)
    da, a1 = lax.optimization_barrier((d, a1))
    a2 = row((f32(da[6 * B :, :, :H]) + a1[2 * B :]).astype(BF16), 3)
    db, b1 = lax.optimization_barrier((d, b1))
    b2 = row((f32(db[2 * B : 4 * B, :, H:]) + b1[: 2 * B]).astype(BF16), 1)
    d, a2, b2, *cols = lax.optimization_barrier((d, a2, b2, *cols))
    own = jnp.concatenate(
        [f32(d[: 2 * B, :, :H]) + a1[: 2 * B] + a2, f32(d[: 2 * B, :, H:]) + b1[2 * B :] + b2], axis=2
    )
    y = row(own[B:].astype(BF16), 4)
    return (own[:B] + y).astype(BF16), *cols


def local(integrals, occ_coef, virt_coef, pair_index):
    r = lax.axis_index("row")
    c = lax.axis_index("col")
    yh, x = r // 4, r % 4
    z, yl, core = c // 4, (c // 2) % 2, c % 2

    pos = jnp.arange(96, dtype=jnp.int32)
    source = ((yh ^ ((pos // B) % 2)) * 4 + (x ^ (pos // (2 * B)))) * B + pos % B
    occ = select_cols(occ_coef, source)

    products, held = {}, occ
    for name, (lo, hi) in CHUNKS.items():
        weights = lax.optimization_barrier((occ, held))[0]
        d = jnp.einsum("mi,mnp->inp", weights, integrals[:, lo:hi], preferred_element_type=F32).astype(BF16)
        products[name] = held = rowmajor(d)
    products["r"], virt_coef, _ = lax.optimization_barrier((products["r"], virt_coef, held))

    apos = jnp.arange(4 * A_BLK, dtype=jnp.int32)
    a_source = ((yl ^ ((apos // A_BLK) % 2)) * 2 + (core ^ (apos // (2 * A_BLK)))) * A_BLK + apos % A_BLK
    virt = {}
    for k in (0, 1, 3, 2):
        v = lax.dynamic_slice_in_dim(virt_coef, (z ^ k) * 4 * A_BLK, 4 * A_BLK, axis=1)
        v = select_cols(v, a_source)
        virt[k] = v if k == 0 else lax.ppermute(v, "col", col_xor(4 * k))

    cols = {n: jnp.concatenate([virt[k][lo:hi] for k in (0, 1, 3, 2)], axis=0) for n, (lo, hi) in CHUNKS.items()}

    halves = {}
    for name, d in products.items():
        if name == "q":
            halves[name], *tied = x_first(d, list(cols.values()))
            cols = dict(zip(cols, tied))
        else:
            halves[name] = x_first(d, [])[0]
    acc = 0.0
    for name, half in halves.items():
        acc = acc + jnp.einsum("inp,na->iap", gather_z(half), cols[name], preferred_element_type=F32)

    r4 = lax.ppermute(acc[:, 2 * A_BLK :].astype(BF16), "col", col_xor(1))
    r5 = lax.ppermute((acc[:, A_BLK : 2 * A_BLK] + r4[:, A_BLK:]).astype(BF16), "col", col_xor(2))
    slab = (acc[:, :A_BLK] + r4[:, :A_BLK] + r5).astype(BF16)
    hot = (lax.broadcasted_iota(jnp.int32, (256, 256), 0) == pair_index[None, :]).astype(BF16)
    return jnp.einsum("iap,pk->iak", slab, hot, preferred_element_type=F32).astype(BF16)


def solution(mesh):
    return jax.shard_map(
        local,
        mesh=mesh,
        in_specs=(P("row", "col", None), P("row", None), P("col", None), P()),
        out_specs=P("row", "col", None),
        check_vma=False,
    )
```

```python
import jax
import jax.numpy as jnp
from jax import lax
from jax.experimental.layout import Layout, with_layout_constraint
from jax.sharding import PartitionSpec as P


F32, BF16 = jnp.float32, jnp.bfloat16
B = 12
A_BLK = 144
H = 128
CHUNKS = {"p": (0, 48), "r": (48, 104), "q": (104, 150)}


def row_perm(mask):
    return [(i, i ^ mask) for i in range(8)]


def col_xor(mask):
    return [(i, i ^ mask) for i in range(16)]


def rowmajor(v):
    return with_layout_constraint(v, Layout(major_to_minor=tuple(range(v.ndim))))


def row(v, mask):
    return lax.ppermute(v, "row", row_perm(mask))


def select_cols(mat, source):
    hot = (lax.broadcasted_iota(jnp.int32, (mat.shape[1], source.shape[0]), 0) == source[None, :]).astype(BF16)
    return jnp.dot(mat, hot, preferred_element_type=F32).astype(BF16)


def gather_z(half):
    return jnp.concatenate([half] + [lax.ppermute(half, "col", col_xor(4 * k)) for k in (1, 3, 2)], axis=1)


def f32(v):
    return v.astype(F32)


def x_first(d, cols, later=()):
    a1 = row(d[2 * B : 6 * B, :, :H], 1)
    b1 = row(d[4 * B :, :, H:], 3)
    da, a1 = lax.optimization_barrier((d, a1))
    a2 = row((f32(da[6 * B :, :, :H]) + a1[2 * B :]).astype(BF16), 3)
    db, b1 = lax.optimization_barrier((d, b1))
    sb = (f32(db[2 * B : 4 * B, :, H:]) + b1[: 2 * B]).astype(BF16)
    sb, *later = lax.optimization_barrier((sb, *later))
    b2 = row(sb, 1)
    d, a2, b2, *cols = lax.optimization_barrier((d, a2, b2, *cols))
    own = jnp.concatenate(
        [f32(d[: 2 * B, :, :H]) + a1[: 2 * B] + a2, f32(d[: 2 * B, :, H:]) + b1[2 * B :] + b2], axis=2
    )
    y = row(own[B:].astype(BF16), 4)
    return (own[:B] + y).astype(BF16), cols, later


def local(integrals, occ_coef, virt_coef, pair_index):
    r = lax.axis_index("row")
    c = lax.axis_index("col")
    yh, x = r // 4, r % 4
    z, yl, core = c // 4, (c // 2) % 2, c % 2

    pos = jnp.arange(96, dtype=jnp.int32)
    source = ((yh ^ ((pos // B) % 2)) * 4 + (x ^ (pos // (2 * B)))) * B + pos % B
    occ = select_cols(occ_coef, source)

    products, held = {}, occ
    for name, (lo, hi) in CHUNKS.items():
        weights = lax.optimization_barrier((occ, held))[0]
        d = jnp.einsum("mi,mnp->inp", weights, integrals[:, lo:hi], preferred_element_type=F32).astype(BF16)
        products[name] = held = rowmajor(d)
    products["r"], _ = lax.optimization_barrier((products["r"], held))
    halves = {}
    halves["p"], _, (virt_coef, products["q"]) = x_first(products["p"], [], [virt_coef, products["q"]])

    apos = jnp.arange(4 * A_BLK, dtype=jnp.int32)
    a_source = ((yl ^ ((apos // A_BLK) % 2)) * 2 + (core ^ (apos // (2 * A_BLK)))) * A_BLK + apos % A_BLK
    virt = {}
    for k in (0, 1, 3, 2):
        v = lax.dynamic_slice_in_dim(virt_coef, (z ^ k) * 4 * A_BLK, 4 * A_BLK, axis=1)
        v = select_cols(v, a_source)
        virt[k] = v if k == 0 else lax.ppermute(v, "col", col_xor(4 * k))

    cols = {n: jnp.concatenate([virt[k][lo:hi] for k in (0, 1, 3, 2)], axis=0) for n, (lo, hi) in CHUNKS.items()}

    halves["r"] = x_first(products["r"], [])[0]
    halves["q"], tied, _ = x_first(products["q"], list(cols.values()))
    cols = dict(zip(cols, tied))
    acc = 0.0
    for name, half in halves.items():
        acc = acc + jnp.einsum("inp,na->iap", gather_z(half), cols[name], preferred_element_type=F32)

    r4 = lax.ppermute(acc[:, 2 * A_BLK :].astype(BF16), "col", col_xor(1))
    r5 = lax.ppermute((acc[:, A_BLK : 2 * A_BLK] + r4[:, A_BLK:]).astype(BF16), "col", col_xor(2))
    slab = (acc[:, :A_BLK] + r4[:, :A_BLK] + r5).astype(BF16)
    hot = (lax.broadcasted_iota(jnp.int32, (256, 256), 0) == pair_index[None, :]).astype(BF16)
    return jnp.einsum("iap,pk->iak", slab, hot, preferred_element_type=F32).astype(BF16)


def solution(mesh):
    return jax.shard_map(
        local,
        mesh=mesh,
        in_specs=(P("row", "col", None), P("row", None), P("col", None), P()),
        out_specs=P("row", "col", None),
        check_vma=False,
    )
```
